32 devices in a mesh: seq: 4 (over z), head: 4 (over y, core), batch: 2 (over x).
Axes of the slice: x: 2, y: 2, z: 4, core: 2. Of those that a mesh axis runs over, the one named last changes fastest.
Arguments:
- tokens: bfloat16 [8192, 2048], P(('batch', 'seq')), parts along dimension 0, may hold values from -6 to 6
- neighbor_bank: bfloat16 [128, 256, 2048], P(('batch', 'seq')), parts along dimension 0, may hold values from -2100 to 2100
- slots: int32 [128], P(('batch', 'seq')), parts along dimension 0, may hold values from 0 to 15
- w_query: bfloat16 [2048, 2048], P('seq', 'head'), may hold values from -0.125 to 0.125
- w_key: bfloat16 [2048, 2048], P('seq', 'head'), may hold values from -0.125 to 0.125
- w_value: bfloat16 [2048, 2048], P('seq', 'head'), may hold values from -0.125 to 0.125
- w_out: bfloat16 [2048, 2048], P('head', 'seq'), may hold values from -0.125 to 0.125
Outputs:
- cross_out: bfloat16 [8192, 2048], P(('batch', 'seq'), 'head'), parts along dimension 0
The draws below stay inside these ranges and needn't reach their ends.
There are 2 independent parts, one for each index of `batch`. The reference program is written for one: setup_inputs(seed, part) draws one part's arguments, and reference() takes and returns one part's arrays. A program takes and returns all parts, laid end to end along the dimension named above; an argument that names none is the same for every part. Nothing has to cross between parts.
Inputs may be any that keep to these rules, and one draw needn't show every extreme that they name: Entry c picks row c // 16 * 16 + slots[c] of neighbor_bank.
All inputs are finite; a program needn't handle non-finite values.
Results may differ from the reference program's by a relative error of at most 0.006.
The reference program's roundings to bfloat16 on the way (of `normed`, `queries`, `retrieved`, `weights` and `attended`) count: a program that leaves them out, or rounds other values in their place, can miss the bound.
Values may be sent and summed in bfloat16 or wider, within the bound.
A program may use at most 128 MiB of HBM per device.

```python
import math
import jax
import jax.numpy as jnp
from jax import lax

D = 2048
HEADS = 16
HEAD_DIM = 128
BLOCK = 64
NEIGHBORS = 2
NEIGH_LEN = 128
BLOCK_DEV = 16
TOKENS = 4096
BLOCKS = 64


def draw_neighbor_bank(key, part):
    key_base = jax.random.fold_in(jax.random.fold_in(key, 11), 0)
    rows = NEIGHBORS * NEIGH_LEN
    base = jnp.clip(jax.random.normal(key_base, (BLOCKS, rows, D), jnp.float32) * 2.0, -8.0, 8.0)
    return base.astype(jnp.bfloat16)


def plant(drawn, own_key, low, largest):
    dims = drawn.shape
    spot = [jax.random.randint(jax.random.fold_in(own_key, axis), (), 0, dims[axis]) for axis in range(len(dims))]
    drawn = drawn.at[tuple(spot)].set(low)
    longest = dims.index(max(dims))
    spot[longest] = (spot[longest] + 1) % dims[longest]
    return drawn.at[tuple(spot)].set(largest)


def block_scale(rng, extent, cuts, smallest, high):
    def one(dim, parts):
        steps = jax.random.uniform(jax.random.fold_in(jax.random.fold_in(rng, 6), dim), (parts,), jnp.float32, smallest / len(cuts), high / len(cuts))
        return jnp.repeat(jnp.exp(steps), extent[dim] // parts).reshape((-1,) + (1,) * (len(extent) - dim - 1))

    loudness = one(*cuts[0])
    for cut in cuts[1:]:
        loudness = loudness * one(*cut)
    return loudness


def noise(key, dims, scale, reach, cuts=(), kind=jnp.bfloat16):
    entries = jax.random.normal(key, dims, jnp.float32) * scale
    if len(cuts) > 0:
        entries = block_scale(key, dims, cuts, -0.22, 0.18) * entries
    return jnp.clip(entries, min=-reach, max=reach).astype(kind)


def setup_inputs(seed: int = 0, part: int = 0) -> dict:
    streams_of = jax.random.split(jax.random.key(seed), 8)
    part_splits = jax.random.split(jax.random.fold_in(streams_of[7], part), 8)
    tokens = noise(part_splits[0], (TOKENS, D), 1.0, 6.0, ((0, 4),))
    neighbor_bank = draw_neighbor_bank(jax.random.fold_in(jax.random.fold_in(streams_of[7], part), 71), part)
    slots = plant(jax.random.randint(part_splits[2], (BLOCKS,), 0, BLOCK_DEV), jax.random.fold_in(part_splits[2], 1), 0, BLOCK_DEV - 1).astype(jnp.int32)
    w_query = noise(streams_of[3], (D, D), D ** -0.5, 0.125, ((0, 4), (1, 4)))
    w_key = noise(streams_of[4], (D, D), D ** -0.5, 0.125, ((0, 4), (1, 4)))
    w_value = noise(streams_of[5], (D, D), D ** -0.5, 0.125, ((0, 4), (1, 4)))
    w_out = noise(streams_of[6], (D, D), D ** -0.5, 0.125, ((0, 4), (1, 4)))
    return {"tokens": tokens, "neighbor_bank": neighbor_bank, "slots": slots, "w_query": w_query, "w_key": w_key, "w_value": w_value, "w_out": w_out}


def rms_normed(tokens):
    hidden = tokens.astype(jnp.float32)
    scale_row = lax.rsqrt(lax.optimization_barrier(jnp.mean(hidden * hidden, axis=-1, keepdims=True)) + 1e-06)
    return (hidden * scale_row).astype(jnp.bfloat16)

def reference(tokens, neighbor_bank, slots, w_query, w_key, w_value, w_out):
    normed = rms_normed(tokens)
    queries = jnp.dot(normed, w_query, preferred_element_type=jnp.float32).astype(jnp.bfloat16)
    block_ids = jnp.arange(BLOCKS, dtype=jnp.int32)
    bank_rows = (block_ids // BLOCK_DEV * BLOCK_DEV + slots).astype(jnp.int32)
    retrieved = jnp.take(neighbor_bank, bank_rows, axis=0).reshape(BLOCKS * NEIGHBORS * NEIGH_LEN, D)
    key_rows = jnp.dot(retrieved, w_key, preferred_element_type=jnp.float32).astype(jnp.bfloat16)
    value_rows = jnp.dot(retrieved, w_value, preferred_element_type=jnp.float32).astype(jnp.bfloat16)
    key_rows = key_rows.reshape(BLOCKS, NEIGHBORS * NEIGH_LEN, HEADS, HEAD_DIM)
    value_rows = value_rows.reshape(BLOCKS, NEIGHBORS * NEIGH_LEN, HEADS, HEAD_DIM)
    padding = jnp.zeros((1, NEIGHBORS * NEIGH_LEN, HEADS, HEAD_DIM), jnp.bfloat16)
    prior_keys = jnp.concatenate([padding, key_rows[:-1]], axis=0)
    prior_values = jnp.concatenate([padding, value_rows[:-1]], axis=0)
    query_blocks = queries.reshape(BLOCKS, BLOCK, HEADS, HEAD_DIM)
    scores = jnp.einsum('cmhd,cnhd->chmn', query_blocks.astype(jnp.float32), prior_keys.astype(jnp.float32)) / math.sqrt(HEAD_DIM)
    peak_score = lax.optimization_barrier(jnp.max(scores, axis=-1, keepdims=True))
    exponent = jnp.exp(scores - peak_score)
    weights = (exponent / lax.optimization_barrier(jnp.sum(exponent, axis=-1, keepdims=True))).astype(jnp.bfloat16)
    attended = jnp.einsum('chmn,cnhd->cmhd', weights.astype(jnp.float32), prior_values.astype(jnp.float32))
    attended = attended.astype(jnp.bfloat16).reshape(TOKENS, D)
    return jnp.dot(attended, w_out, preferred_element_type=jnp.float32).astype(jnp.bfloat16)
```

```python
import functools
import math

import jax
import jax.numpy as jnp
from jax import lax
from jax.experimental import pallas as pl
from jax.experimental.pallas import tpu as pltpu
from jax.sharding import PartitionSpec as P

HEAD_DIM = 128
F32 = jnp.float32
BF16 = jnp.bfloat16


def fused(S, H, NS, tokens, bank, slots, w_query, w_key, w_value, w_out, out,
          G, WO, tok, normed, rows_in, kv, qb, halo_out, halo_in, att_own, att, acc,
          ld_sem, wl_sem, zr, xr, send_r, send_l, send_x, halo_s, halo_r,
          att_s, att_r, att_l, wo_s, wo_r, wo_xs, wo_xr, wo_l):
    s, h, b = lax.axis_index("seq"), lax.axis_index("head"), lax.axis_index("batch")
    nblk, nrow, D = bank.shape
    T = tokens.shape[0]
    blk = T // nblk
    CW = HEAD_DIM
    RS = w_query.shape[0]
    RH = RS // 2
    WH = CW // 2

    def dev(seq, head, batch):
        return {"seq": seq, "head": head, "batch": batch}

    def rcopy(src, dst, ss, rs, device):
        return pltpu.make_async_remote_copy(
            src_ref=src, dst_ref=dst, send_sem=ss, recv_sem=rs,
            device_id=device, device_id_type=pl.DeviceIdType.MESH)

    w_loads = []
    for k, w in enumerate((w_query, w_key, w_value)):
        for j in range(NS):
            c = pltpu.make_async_copy(
                w.at[:, pl.ds(j * CW, CW)],
                G.at[j, pl.ds(s * RS, RS), pl.ds(k * CW, CW)], wl_sem.at[k * NS + j])
            c.start()
            w_loads.append(c)
    tok_load = pltpu.make_async_copy(tokens, tok, ld_sem.at[nblk])
    tok_load.start()
    bank_loads = [pltpu.make_async_copy(bank.at[i], rows_in.at[i], ld_sem.at[i]) for i in range(nblk)]
    for c in bank_loads:
        c.start()

    barrier = pltpu.get_barrier_semaphore()
    for i in range(S):
        for k in range(H):
            @pl.when(jnp.logical_or(s != i, h != k))
            def _():
                pl.semaphore_signal(barrier, inc=1, device_id=dev(i, k, b), device_id_type=pl.DeviceIdType.MESH)
    pl.semaphore_signal(barrier, inc=1, device_id=dev(s, h, 1 - b), device_id_type=pl.DeviceIdType.MESH)
    pl.semaphore_wait(barrier, S * H)

    def chunk(t, origin, half):
        return G.at[t, pl.ds(origin * RS + half * RH, RH), :]

    def right(t, origin):
        return rcopy(chunk(t, origin, b), chunk(t, origin, b), send_r.at[t, origin], zr.at[t, origin],
                     dev(lax.rem(s + 1, S), h, b))

    def left(t, origin):
        return rcopy(chunk(t, origin, b), chunk(t, origin, b), send_l.at[t, origin], zr.at[t, origin],
                     dev(lax.rem(s + S - 1, S), h, b))

    def twin(t, origin, half):
        return rcopy(chunk(t, origin, half), chunk(t, origin, half), send_x.at[t, origin], xr.at[t, origin],
                     dev(s, h, 1 - b))

    def send_own(t):
        @pl.when(s < S - 1)
        def _():
            right(t, s).start()

        @pl.when(s > 0)
        def _():
            left(t, s).start()

    def relay(t, d):
        @pl.when(s >= d)
        def _():
            right(t, s - d).wait_recv()

            @pl.when(s < S - 1)
            def _():
                right(t, s - d).start()
            twin(t, s - d, b).start()

        @pl.when(s + d < S)
        def _():
            left(t, s + d).wait_recv()

            @pl.when(s > 0)
            def _():
                left(t, s + d).start()
            twin(t, s + d, b).start()

    def wo_part(origin, half):
        return WO.at[:, pl.ds(origin * CW + half * WH, WH), :]

    def wo_send(dest):
        return rcopy(w_out.at[:, pl.ds(b * WH, WH), :], wo_part(h, b), wo_s.at[dest], wo_r.at[h],
                     dev(dest, s, b))

    def wo_twin(origin, half):
        return rcopy(wo_part(origin, half), wo_part(origin, half), wo_xs.at[origin], wo_xr.at[origin],
                     dev(s, h, 1 - b))

    wo_own = pltpu.make_async_copy(w_out, WO.at[:, pl.ds(h * CW, CW), :], wo_l)

    def attend(t, first_key, blocks):
        scores, probs = [], []
        for c, keys in blocks:
            q = qb[pl.ds(c * blk, blk), :]
            k = keys(0)
            scores.append(lax.dot_general(q, k, (((1,), (1,)), ((), ())), preferred_element_type=F32)
                          * (1.0 / math.sqrt(HEAD_DIM)))
        for sc in scores:
            e = jnp.exp(sc - jnp.max(sc, axis=-1, keepdims=True))
            probs.append((e / jnp.sum(e, axis=-1, keepdims=True)).astype(BF16))
        for (c, keys), p in zip(blocks, probs):
            o = jnp.dot(p, keys(1), preferred_element_type=F32)
            att_own[t, pl.ds(c * blk, blk), :] = o.astype(BF16)

    def halo(t):
        return rcopy(halo_out.at[t], halo_in.at[t], halo_s.at[t], halo_r.at[t], dev(lax.rem(s + 1, S), h, b))

    peers = ((h // 2) * 2 + 1 - lax.rem(h, 2), lax.rem(h + 2, H), lax.rem((h // 2) * 2 + 1 - lax.rem(h, 2) + 2, H))

    def att_send(t, k):
        return rcopy(att_own.at[t], att.at[t, :, pl.ds(h * CW, CW)], att_s.at[t, k], att_r.at[t, k],
                     dev(s, peers[k], b))

    def att_here(t):
        return pltpu.make_async_copy(att_own.at[t], att.at[t, :, pl.ds(h * CW, CW)], att_l.at[t])

    per = 4 if nblk % 4 == 0 else 1
    steps = nblk // per

    def project(t, lo, hi):
        def one(i, _):
            rows = rows_in[pl.ds(i * per, per)].reshape(per * nrow, D)
            kv[pl.ds(i * per, per)] = jnp.dot(
                rows, G[t, :, pl.ds(CW, 2 * CW)], preferred_element_type=F32).astype(BF16).reshape(per, nrow, 2 * CW)
            return 0
        lax.fori_loop(lo, hi, one, 0)

    def queries(t):
        qb[...] = jnp.dot(normed[...], G[t, :, pl.ds(0, CW)], preferred_element_type=F32).astype(BF16)

    for c in w_loads:
        c.wait()
    send_own(0)

    @pl.when(s == 0)
    def _():
        halo_in[...] = jnp.zeros_like(halo_in)

    tok_load.wait()

    def norm(i, _):
        x = tok[pl.ds(i * blk, blk), :].astype(F32)
        normed[pl.ds(i * blk, blk), :] = (
            x * lax.rsqrt(jnp.mean(x * x, axis=-1, keepdims=True) + 1e-06)).astype(BF16)
        return 0
    lax.fori_loop(0, nblk, norm, 0)

    @pl.when(h == s)
    def _():
        wo_own.start()
    for c in bank_loads:
        c.wait()

    group = max(g for g in range(1, 6) if (nblk - 1) % g == 0)

    def stage(t, _):
        @pl.when(t < NS - 1)
        def _():
            send_own(t + 1)

        @pl.when(t < S)
        def _():
            dest = lax.rem(t * (S - 1), S)

            @pl.when(jnp.logical_or(dest != s, h != s))
            def _():
                wo_send(dest).start()

        @pl.when(t < NS)
        def _():
            relay(t, 1)

        @pl.when(t == NS)
        def _():
            for o in range(H):
                @pl.when(jnp.logical_or(s != h, h != o))
                def _():
                    rcopy(wo_part(o, b), wo_part(o, b), wo_s.at[0], wo_r.at[o], dev(s, h, 1 - b)).wait_recv()
                    wo_twin(o, b).start()

        @pl.when(t > 0)
        def _():
            project(t - 1, 0, steps // 2)

        @pl.when(t < NS)
        def _():
            relay(t, 2)

        @pl.when(t > 0)
        def _():
            project(t - 1, steps // 2, steps)
            last = slots[nblk - 1]

            @pl.when(s < S - 1)
            def _():
                halo_out[t - 1] = kv[last]
                halo(t - 1).start()
            queries(t - 1)

        @pl.when(t < NS)
        def _():
            for d in range(3, S):
                relay(t, d)

        @pl.when(t > 0)
        def _():
            u = t - 1

            def some(i, _):
                blocks = []
                for g in range(group):
                    c = 1 + i * group + g
                    at = slots[c - 1]
                    blocks.append((c, lambda k, at=at: kv[at, :, k * CW:(k + 1) * CW]))
                attend(u, None, blocks)
                return 0
            lax.fori_loop(0, (nblk - 1) // group, some, 0)

            @pl.when(s > 0)
            def _():
                halo(u).wait_recv()
            attend(u, None, [(0, lambda k: halo_in[u, :, k * CW:(k + 1) * CW])])
            for k in range(3):
                att_send(u, k).start()
            att_here(u).start()

        @pl.when(t < NS)
        def _():
            for o in range(S):
                @pl.when(s != o)
                def _():
                    twin(t, o, 1 - b).wait_recv()
        return 0

    lax.fori_loop(0, NS + 1, stage, 0)

    for o in range(H):
        @pl.when(jnp.logical_or(s != h, h != o))
        def _():
            wo_twin(o, 1 - b).wait_recv()

    @pl.when(h == s)
    def _():
        wo_own.wait()

    tile = T // 4

    def fold(j, _):
        att_here(j).wait()
        for k in range(3):
            rcopy(att_own.at[j], att.at[j, :, pl.ds(peers[k] * CW, CW)], att_s.at[j, k], att_r.at[j, k],
                  dev(s, peers[k], b)).wait_recv()

        def rows(i, _):
            r = pl.ds(i * tile, tile)
            part = jnp.dot(att[j, r, :], WO[j], preferred_element_type=F32)

            @pl.when(j == 0)
            def _():
                acc[r, :] = part

            @pl.when(jnp.logical_and(j > 0, j < NS - 1))
            def _():
                acc[r, :] += part

            @pl.when(j == NS - 1)
            def _():
                out[r, :] = (acc[r, :] + part).astype(BF16)
            return 0
        lax.fori_loop(0, 4, rows, 0)
        return 0
    lax.fori_loop(0, NS, fold, 0)

    def drain(t, _):
        for d in range(S):
            @pl.when(jnp.logical_and(s >= d, s < S - 1))
            def _():
                right(t, s - d).wait_send()

            @pl.when(jnp.logical_and(s + d < S, s > 0))
            def _():
                left(t, s + d).wait_send()
        for o in range(S):
            @pl.when(s != o)
            def _():
                twin(t, o, b).wait_send()

        @pl.when(s < S - 1)
        def _():
            halo(t).wait_send()
        for k in range(3):
            att_send(t, k).wait_send()
        return 0
    lax.fori_loop(0, NS, drain, 0)
    for dest in range(S):
        @pl.when(jnp.logical_or(dest != s, h != s))
        def _():
            wo_send(dest).wait_send()
    for o in range(H):
        @pl.when(jnp.logical_or(s != h, h != o))
        def _():
            wo_twin(o, b).wait_send()


def one_kernel(tokens, neighbor_bank, slots, w_query, w_key, w_value, w_out):
    S, H = lax.axis_size("seq"), lax.axis_size("head")
    T, D = tokens.shape
    nblk, nrow = neighbor_bank.shape[:2]
    width = w_query.shape[1]
    NS = width // HEAD_DIM
    CW = HEAD_DIM
    out_cols = D // H
    dma = pltpu.SemaphoreType.DMA
    hbm = pl.BlockSpec(memory_space=pl.ANY)
    return pl.pallas_call(
        functools.partial(fused, S, H, NS),
        out_shape=jax.ShapeDtypeStruct((T, out_cols), BF16),
        in_specs=[hbm, hbm, pl.BlockSpec(memory_space=pltpu.SMEM), hbm, hbm, hbm, hbm],
        out_specs=pl.BlockSpec(memory_space=pltpu.VMEM),
        scratch_shapes=[
            pltpu.VMEM((NS, D, 3 * CW), BF16),
            pltpu.VMEM((NS, H * CW, out_cols), BF16),
            pltpu.VMEM((T, D), BF16),
            pltpu.VMEM((T, D), BF16),
            pltpu.VMEM((nblk, nrow, D), BF16),
            pltpu.VMEM((nblk, nrow, 2 * CW), BF16),
            pltpu.VMEM((T, CW), BF16),
            pltpu.VMEM((NS, nrow, 2 * CW), BF16),
            pltpu.VMEM((NS, nrow, 2 * CW), BF16),
            pltpu.VMEM((NS, T, CW), BF16),
            pltpu.VMEM((NS, T, H * CW), BF16),
            pltpu.VMEM((T, out_cols), F32),
            dma((nblk + 1,)),
            dma((3 * NS,)),
            dma((NS, S)), dma((NS, S)), dma((NS, S)), dma((NS, S)), dma((NS, S)),
            dma((NS,)), dma((NS,)),
            dma((NS, 3)), dma((NS, 3)), dma((NS,)),
            dma((S,)), dma((H,)), dma((H,)), dma((H,)), dma,
        ],
        compiler_params=pltpu.CompilerParams(
            collective_id=0, has_side_effects=True, vmem_limit_bytes=63 * 1024 * 1024),
    )(tokens, neighbor_bank, slots, w_query, w_key, w_value, w_out.reshape(NS, CW, -1))


def passed_along(block, axis, distance):
    devices = range(lax.axis_size(axis))
    route = [(i - distance, i) for i in devices if i - distance in devices]
    return lax.ppermute(block, axis, route)


def attend(query_blocks, key_blocks, value_blocks):
    scores = jnp.einsum(
        "cmhd,cnhd->chmn", query_blocks, key_blocks, preferred_element_type=jnp.float32
    ) / math.sqrt(HEAD_DIM)
    peak_score = jnp.max(scores, axis=-1, keepdims=True)
    exponent = jnp.exp(scores - peak_score)
    weights = (exponent / jnp.sum(exponent, axis=-1, keepdims=True)).astype(jnp.bfloat16)
    blended = jnp.einsum(
        "chmn,cnhd->cmhd", weights, value_blocks, preferred_element_type=jnp.float32
    ).astype(jnp.bfloat16)
    return blended.reshape(blended.shape[0] * blended.shape[1], blended.shape[2] * blended.shape[3])


def fold_rows(source, shard_rows):
    return jnp.dot(source, shard_rows, preferred_element_type=jnp.float32)


def local(tokens, neighbor_bank, slots, w_query, w_key, w_value, w_out):
    tok_rows, model_width = tokens.shape
    block_count = neighbor_bank.shape[0]
    neighbor_rows = neighbor_bank.shape[1]
    block_len = tok_rows // block_count
    local_width = w_query.shape[1]
    local_heads = local_width // HEAD_DIM
    hidden = tokens.astype(jnp.float32)
    normed = (hidden * lax.rsqrt(jnp.mean(hidden * hidden, axis=-1, keepdims=True) + 1e-06)).astype(
        jnp.bfloat16
    )
    retrieved = jnp.take(neighbor_bank, slots, axis=0)
    arrived = passed_along(retrieved[block_count - 1], "seq", 1)
    context = jnp.concatenate([arrived[None], retrieved[: block_count - 1]], axis=0)
    context_flat = context.reshape(block_count * neighbor_rows, model_width)
    query_sum = fold_rows(normed, lax.all_gather(w_query, "seq", axis=0, tiled=True))
    key_sum = fold_rows(context_flat, lax.all_gather(w_key, "seq", axis=0, tiled=True))
    value_sum = fold_rows(context_flat, lax.all_gather(w_value, "seq", axis=0, tiled=True))
    query_blocks = query_sum.astype(jnp.bfloat16).reshape(
        block_count, block_len, local_heads, HEAD_DIM
    )
    key_blocks = key_sum.astype(jnp.bfloat16).reshape(
        block_count, neighbor_rows, local_heads, HEAD_DIM
    )
    value_blocks = value_sum.astype(jnp.bfloat16).reshape(
        block_count, neighbor_rows, local_heads, HEAD_DIM
    )
    attended = attend(query_blocks, key_blocks, value_blocks)
    every_head = lax.all_gather(attended, "head", axis=1, tiled=True)
    wide_rows = lax.all_gather(w_out, "seq", axis=1, tiled=True)
    own_columns = lax.all_to_all(wide_rows, "head", split_axis=1, concat_axis=0, tiled=True)
    return jnp.dot(every_head, own_columns, preferred_element_type=jnp.float32).astype(jnp.bfloat16)


def solution(mesh):
    in_specs = (
        P(("batch", "seq"), None),
        P(("batch", "seq"), None, None),
        P(("batch", "seq")),
        P("seq", "head"),
        P("seq", "head"),
        P("seq", "head"),
        P("head", "seq"),
    )
    out_specs = P(("batch", "seq"), "head")
    square = mesh.shape["seq"] == 4 and mesh.shape["head"] == 4 and mesh.shape["batch"] == 2
    body = one_kernel if square else local
    return jax.shard_map(body, mesh=mesh, in_specs=in_specs, out_specs=out_specs, check_vma=False)
```

```python
import functools
import math

import jax
import jax.numpy as jnp
from jax import lax
from jax.experimental import pallas as pl
from jax.experimental.pallas import tpu as pltpu
from jax.sharding import PartitionSpec as P

HEAD_DIM = 128
F32 = jnp.float32
BF16 = jnp.bfloat16


def fused(S, H, NS, tokens, bank, slots, w_query, w_key, w_value, w_out, out,
          G, WO, tok, normed, rows_in, kv, qb, halo_out, halo_in, att_own, att, acc,
          ld_sem, wl_sem, zr, xr, send_r, send_l, send_x, halo_s, halo_r,
          att_s, att_r, att_l, wo_s, wo_r, wo_l):
    s, h, b = lax.axis_index("seq"), lax.axis_index("head"), lax.axis_index("batch")
    nblk, nrow, D = bank.shape
    T = tokens.shape[0]
    blk = T // nblk
    CW = HEAD_DIM
    RS = w_query.shape[0]
    RH = RS // 2
    WH = CW // 2

    def dev(seq, head, batch):
        return {"seq": seq, "head": head, "batch": batch}

    def rcopy(src, dst, ss, rs, device):
        return pltpu.make_async_remote_copy(
            src_ref=src, dst_ref=dst, send_sem=ss, recv_sem=rs,
            device_id=device, device_id_type=pl.DeviceIdType.MESH)

    w_loads = []
    for k, w in enumerate((w_query, w_key, w_value)):
        for j in range(NS):
            c = pltpu.make_async_copy(
                w.at[:, pl.ds(j * CW, CW)],
                G.at[j, pl.ds(s * RS, RS), pl.ds(k * CW, CW)], wl_sem.at[k * NS + j])
            c.start()
            w_loads.append(c)
    tok_load = pltpu.make_async_copy(tokens, tok, ld_sem.at[nblk])
    tok_load.start()
    bank_loads = [pltpu.make_async_copy(bank.at[i], rows_in.at[i], ld_sem.at[i]) for i in range(nblk)]
    for c in bank_loads:
        c.start()

    barrier = pltpu.get_barrier_semaphore()
    for i in range(S):
        for k in range(H):
            @pl.when(jnp.logical_or(s != i, h != k))
            def _():
                pl.semaphore_signal(barrier, inc=1, device_id=dev(i, k, b), device_id_type=pl.DeviceIdType.MESH)
    pl.semaphore_signal(barrier, inc=1, device_id=dev(s, h, 1 - b), device_id_type=pl.DeviceIdType.MESH)
    pl.semaphore_wait(barrier, S * H)

    def chunk(t, origin, half):
        if isinstance(t, int) and t == NS:
            return wo_part(origin, half)
        return G.at[t, pl.ds(origin * RS + half * RH, RH), :]

    def right(t, origin):
        return rcopy(chunk(t, origin, b), chunk(t, origin, b), send_r.at[t, origin], zr.at[t, origin],
                     dev(lax.rem(s + 1, S), h, b))

    def left(t, origin):
        return rcopy(chunk(t, origin, b), chunk(t, origin, b), send_l.at[t, origin], zr.at[t, origin],
                     dev(lax.rem(s + S - 1, S), h, b))

    def twin(t, origin, half):
        return rcopy(chunk(t, origin, half), chunk(t, origin, half), send_x.at[t, origin], xr.at[t, origin],
                     dev(s, h, 1 - b))

    def send_own(t):
        @pl.when(s < S - 1)
        def _():
            right(t, s).start()

        @pl.when(s > 0)
        def _():
            left(t, s).start()

    def relay(t, d):
        @pl.when(s >= d)
        def _():
            right(t, s - d).wait_recv()

            @pl.when(s < S - 1)
            def _():
                right(t, s - d).start()
            twin(t, s - d, b).start()

        @pl.when(s + d < S)
        def _():
            left(t, s + d).wait_recv()

            @pl.when(s > 0)
            def _():
                left(t, s + d).start()
            twin(t, s + d, b).start()

    def wo_part(origin, half):
        return WO.at[:, pl.ds(origin * CW + half * WH, WH), :]

    def wo_turn(origin, device):
        return rcopy(w_out.at[:, pl.ds(b * WH, WH), :], wo_part(origin, b), wo_s, wo_r, device)

    wo_own = pltpu.make_async_copy(w_out, WO.at[:, pl.ds(h * CW, CW), :], wo_l)

    def attend(t, first_key, blocks):
        scores, probs = [], []
        for c, keys in blocks:
            q = qb[pl.ds(c * blk, blk), :]
            k = keys(0)
            scores.append(lax.dot_general(q, k, (((1,), (1,)), ((), ())), preferred_element_type=F32)
                          * (1.0 / math.sqrt(HEAD_DIM)))
        for sc in scores:
            e = jnp.exp(sc - jnp.max(sc, axis=-1, keepdims=True))
            probs.append((e / jnp.sum(e, axis=-1, keepdims=True)).astype(BF16))
        for (c, keys), p in zip(blocks, probs):
            o = jnp.dot(p, keys(1), preferred_element_type=F32)
            att_own[t, pl.ds(c * blk, blk), :] = o.astype(BF16)

    def halo(t):
        return rcopy(halo_out.at[t], halo_in.at[t], halo_s.at[t], halo_r.at[t], dev(lax.rem(s + 1, S), h, b))

    peers = ((h // 2) * 2 + 1 - lax.rem(h, 2), lax.rem(h + 2, H), lax.rem((h // 2) * 2 + 1 - lax.rem(h, 2) + 2, H))

    def att_send(t, k):
        return rcopy(att_own.at[t], att.at[t, :, pl.ds(h * CW, CW)], att_s.at[t, k], att_r.at[t, k],
                     dev(s, peers[k], b))

    def att_here(t):
        return pltpu.make_async_copy(att_own.at[t], att.at[t, :, pl.ds(h * CW, CW)], att_l.at[t])

    per = 4 if nblk % 4 == 0 else 1
    steps = nblk // per

    def project(t, lo, hi):
        def one(i, _):
            rows = rows_in[pl.ds(i * per, per)].reshape(per * nrow, D)
            kv[pl.ds(i * per, per)] = jnp.dot(
                rows, G[t, :, pl.ds(CW, 2 * CW)], preferred_element_type=F32).astype(BF16).reshape(per, nrow, 2 * CW)
            return 0
        lax.fori_loop(lo, hi, one, 0)

    def queries(t):
        qb[...] = jnp.dot(normed[...], G[t, :, pl.ds(0, CW)], preferred_element_type=F32).astype(BF16)

    for c in w_loads:
        c.wait()
    @pl.when(h != s)
    def _():
        wo_turn(h, dev(h, s, b)).start()

    @pl.when(h == s)
    def _():
        wo_own.start()
        wo_own.wait()
    send_own(0)
    send_own(1)

    @pl.when(s == 0)
    def _():
        halo_in[...] = jnp.zeros_like(halo_in)

    tok_load.wait()

    def norm(i, _):
        x = tok[pl.ds(i * blk, blk), :].astype(F32)
        normed[pl.ds(i * blk, blk), :] = (
            x * lax.rsqrt(jnp.mean(x * x, axis=-1, keepdims=True) + 1e-06)).astype(BF16)
        return 0
    lax.fori_loop(0, nblk, norm, 0)

    for c in bank_loads:
        c.wait()

    group = max(g for g in range(1, 6) if (nblk - 1) % g == 0)

    def stage(t, _):
        @pl.when(t < NS - 2)
        def _():
            send_own(t + 2)

        @pl.when(t < NS)
        def _():
            relay(t, 1)

        @pl.when(t > 0)
        def _():
            for o in range(S):
                @pl.when(s != o)
                def _():
                    twin(t - 1, o, 1 - b).wait_recv()
            project(t - 1, 0, steps // 2)

        @pl.when(t < NS)
        def _():
            relay(t, 2)

        @pl.when(t > 0)
        def _():
            project(t - 1, steps // 2, steps)
            last = slots[nblk - 1]

            @pl.when(s < S - 1)
            def _():
                halo_out[t - 1] = kv[last]
                halo(t - 1).start()
            queries(t - 1)

        @pl.when(t < NS)
        def _():
            for d in range(3, S):
                relay(t, d)

        @pl.when(t == 0)
        def _():
            @pl.when(h != s)
            def _():
                wo_turn(s, dev(h, s, b)).wait_recv()
                twin(NS, s, b).start()
            send_own(NS)

        for d in range(1, S):
            @pl.when(t == d)
            def _():
                relay(NS, d)

        @pl.when(t > 0)
        def _():
            u = t - 1

            def some(i, _):
                blocks = []
                for g in range(group):
                    c = 1 + i * group + g
                    at = slots[c - 1]
                    blocks.append((c, lambda k, at=at: kv[at, :, k * CW:(k + 1) * CW]))
                attend(u, None, blocks)
                return 0
            lax.fori_loop(0, (nblk - 1) // group, some, 0)

            @pl.when(s > 0)
            def _():
                halo(u).wait_recv()
            attend(u, None, [(0, lambda k: halo_in[u, :, k * CW:(k + 1) * CW])])
            for k in range(3):
                att_send(u, k).start()
            att_here(u).start()

        return 0

    lax.fori_loop(0, NS + 1, stage, 0)

    for o in range(S):
        @pl.when(jnp.logical_or(s != o, h != s))
        def _():
            twin(NS, o, 1 - b).wait_recv()

    tile = T // 4

    def fold(j, _):
        att_here(j).wait()
        for k in range(3):
            rcopy(att_own.at[j], att.at[j, :, pl.ds(peers[k] * CW, CW)], att_s.at[j, k], att_r.at[j, k],
                  dev(s, peers[k], b)).wait_recv()

        def rows(i, _):
            r = pl.ds(i * tile, tile)
            part = jnp.dot(att[j, r, :], WO[j], preferred_element_type=F32)

            @pl.when(j == 0)
            def _():
                acc[r, :] = part

            @pl.when(jnp.logical_and(j > 0, j < NS - 1))
            def _():
                acc[r, :] += part

            @pl.when(j == NS - 1)
            def _():
                out[r, :] = (acc[r, :] + part).astype(BF16)
            return 0
        lax.fori_loop(0, 4, rows, 0)
        return 0
    lax.fori_loop(0, NS, fold, 0)

    def drain_weights(t):
        for d in range(S):
            @pl.when(jnp.logical_and(s >= d, s < S - 1))
            def _():
                right(t, s - d).wait_send()

            @pl.when(jnp.logical_and(s + d < S, s > 0))
            def _():
                left(t, s + d).wait_send()
        for o in range(S):
            @pl.when(s != o)
            def _():
                twin(t, o, b).wait_send()

    def drain(t, _):
        drain_weights(t)

        @pl.when(s < S - 1)
        def _():
            halo(t).wait_send()
        for k in range(3):
            att_send(t, k).wait_send()
        return 0
    lax.fori_loop(0, NS, drain, 0)
    drain_weights(NS)

    @pl.when(h != s)
    def _():
        twin(NS, s, b).wait_send()
        wo_turn(h, dev(h, s, b)).wait_send()


def one_kernel(tokens, neighbor_bank, slots, w_query, w_key, w_value, w_out):
    S, H = lax.axis_size("seq"), lax.axis_size("head")
    T, D = tokens.shape
    nblk, nrow = neighbor_bank.shape[:2]
    width = w_query.shape[1]
    NS = width // HEAD_DIM
    CW = HEAD_DIM
    out_cols = D // H
    dma = pltpu.SemaphoreType.DMA
    hbm = pl.BlockSpec(memory_space=pl.ANY)
    return pl.pallas_call(
        functools.partial(fused, S, H, NS),
        out_shape=jax.ShapeDtypeStruct((T, out_cols), BF16),
        in_specs=[hbm, hbm, pl.BlockSpec(memory_space=pltpu.SMEM), hbm, hbm, hbm, hbm],
        out_specs=pl.BlockSpec(memory_space=pltpu.VMEM),
        scratch_shapes=[
            pltpu.VMEM((NS, D, 3 * CW), BF16),
            pltpu.VMEM((NS, H * CW, out_cols), BF16),
            pltpu.VMEM((T, D), BF16),
            pltpu.VMEM((T, D), BF16),
            pltpu.VMEM((nblk, nrow, D), BF16),
            pltpu.VMEM((nblk, nrow, 2 * CW), BF16),
            pltpu.VMEM((T, CW), BF16),
            pltpu.VMEM((NS, nrow, 2 * CW), BF16),
            pltpu.VMEM((NS, nrow, 2 * CW), BF16),
            pltpu.VMEM((NS, T, CW), BF16),
            pltpu.VMEM((NS, T, H * CW), BF16),
            pltpu.VMEM((T, out_cols), F32),
            dma((nblk + 1,)),
            dma((3 * NS,)),
            dma((NS + 1, S)), dma((NS + 1, S)), dma((NS + 1, S)), dma((NS + 1, S)), dma((NS + 1, S)),
            dma((NS,)), dma((NS,)),
            dma((NS, 3)), dma((NS, 3)), dma((NS,)),
            dma, dma, dma,
        ],
        compiler_params=pltpu.CompilerParams(
            collective_id=0, has_side_effects=True, vmem_limit_bytes=63 * 1024 * 1024),
    )(tokens, neighbor_bank, slots, w_query, w_key, w_value, w_out.reshape(NS, CW, -1))


def passed_along(block, axis, distance):
    devices = range(lax.axis_size(axis))
    route = [(i - distance, i) for i in devices if i - distance in devices]
    return lax.ppermute(block, axis, route)


def attend(query_blocks, key_blocks, value_blocks):
    scores = jnp.einsum(
        "cmhd,cnhd->chmn", query_blocks, key_blocks, preferred_element_type=jnp.float32
    ) / math.sqrt(HEAD_DIM)
    peak_score = jnp.max(scores, axis=-1, keepdims=True)
    exponent = jnp.exp(scores - peak_score)
    weights = (exponent / jnp.sum(exponent, axis=-1, keepdims=True)).astype(jnp.bfloat16)
    blended = jnp.einsum(
        "chmn,cnhd->cmhd", weights, value_blocks, preferred_element_type=jnp.float32
    ).astype(jnp.bfloat16)
    return blended.reshape(blended.shape[0] * blended.shape[1], blended.shape[2] * blended.shape[3])


def fold_rows(source, shard_rows):
    return jnp.dot(source, shard_rows, preferred_element_type=jnp.float32)


def local(tokens, neighbor_bank, slots, w_query, w_key, w_value, w_out):
    tok_rows, model_width = tokens.shape
    block_count = neighbor_bank.shape[0]
    neighbor_rows = neighbor_bank.shape[1]
    block_len = tok_rows // block_count
    local_width = w_query.shape[1]
    local_heads = local_width // HEAD_DIM
    hidden = tokens.astype(jnp.float32)
    normed = (hidden * lax.rsqrt(jnp.mean(hidden * hidden, axis=-1, keepdims=True) + 1e-06)).astype(
        jnp.bfloat16
    )
    retrieved = jnp.take(neighbor_bank, slots, axis=0)
    arrived = passed_along(retrieved[block_count - 1], "seq", 1)
    context = jnp.concatenate([arrived[None], retrieved[: block_count - 1]], axis=0)
    context_flat = context.reshape(block_count * neighbor_rows, model_width)
    query_sum = fold_rows(normed, lax.all_gather(w_query, "seq", axis=0, tiled=True))
    key_sum = fold_rows(context_flat, lax.all_gather(w_key, "seq", axis=0, tiled=True))
    value_sum = fold_rows(context_flat, lax.all_gather(w_value, "seq", axis=0, tiled=True))
    query_blocks = query_sum.astype(jnp.bfloat16).reshape(
        block_count, block_len, local_heads, HEAD_DIM
    )
    key_blocks = key_sum.astype(jnp.bfloat16).reshape(
        block_count, neighbor_rows, local_heads, HEAD_DIM
    )
    value_blocks = value_sum.astype(jnp.bfloat16).reshape(
        block_count, neighbor_rows, local_heads, HEAD_DIM
    )
    attended = attend(query_blocks, key_blocks, value_blocks)
    every_head = lax.all_gather(attended, "head", axis=1, tiled=True)
    wide_rows = lax.all_gather(w_out, "seq", axis=1, tiled=True)
    own_columns = lax.all_to_all(wide_rows, "head", split_axis=1, concat_axis=0, tiled=True)
    return jnp.dot(every_head, own_columns, preferred_element_type=jnp.float32).astype(jnp.bfloat16)


def solution(mesh):
    in_specs = (
        P(("batch", "seq"), None),
        P(("batch", "seq"), None, None),
        P(("batch", "seq")),
        P("seq", "head"),
        P("seq", "head"),
        P("seq", "head"),
        P("head", "seq"),
    )
    out_specs = P(("batch", "seq"), "head")
    square = mesh.shape["seq"] == 4 and mesh.shape["head"] == 4 and mesh.shape["batch"] == 2
    body = one_kernel if square else local
    return jax.shard_map(body, mesh=mesh, in_specs=in_specs, out_specs=out_specs, check_vma=False)
```
